256 devices in a mesh: seq: 32 (over z, x), exp: 8 (over y, core).
Axes of the slice: x: 4, y: 4, z: 8, core: 2. Of those that a mesh axis runs over, the one named last changes fastest.
Arguments:
- tokens: bfloat16 [32768, 2560], P(('seq', 'exp')), may hold values from -6 to 6
- routes: int32 [32768, 1], P(('seq', 'exp')), may hold values from 0 to 15; in each aligned block of 128 rows (0 to 127, 128 to 255, ...) at most 16 rows name the same one
- gate_inner_weight: bfloat16 [2560, 2, 3072], P(None, None, 'exp'), may hold values from -0.125 to 0.125
- state_map_weight: bfloat16 [2560, 256], replicated, may hold values from -0.125 to 0.125
- step_size_weight: bfloat16 [2560, 48], P(None, 'exp'), may hold values from -0.125 to 0.125
- adapter_down_weight: bfloat16 [2560, 128], P(None, 'exp'), may hold values from -0.125 to 0.125
- adapter_up_weight: bfloat16 [128, 2, 3072], P(None, None, 'exp'), may hold values from -1.5 to 1.5
- inner_conv_taps: float32 [4, 3072], P(None, 'exp'), may hold values from -3 to 3
- state_map_taps: float32 [4, 256], replicated, may hold values from -3 to 3
- inner_conv_bias: float32 [3072], P('exp'), may hold values from -3 to 3
- state_map_conv_bias: float32 [256], replicated, may hold values from -3 to 3
- step_size_bias: float32 [48], P('exp'), may hold values from -6 to -3
- head_decay_rate: float32 [48], P('exp'), may hold values from 4.656613e-06 to 8
- direct_head_scale: float32 [48], P('exp'), may hold values from 0.5 to 2
- gated_norm_scale: float32 [3072], P('exp'), may hold values from 0.5 to 1.5
Outputs:
- mixed: bfloat16 [32768, 3072], P('seq', 'exp')
The draws below stay inside these ranges and needn't reach their ends.
Inputs may be any that keep to these rules, and one draw needn't show every extreme that they name: `routes`: among the rows of one device no expert is named more than 16 times.
All inputs are finite; a program needn't handle non-finite values.
Results may differ from the reference program's by a relative error of at most 0.0034.
Values may be sent and summed in bfloat16 or wider, within the bound.
A program may use at most 64 MiB of HBM per device.

```python
import math
import jax
import jax.numpy as jnp
import numpy as np
from jax import lax

MODEL_WIDTH = 2560
STATE = 128
HEADDIM = 64
KERNEL = 4
H = 48
ADAPTER_EXPERTS = 16
EXPERT_RANK = 8
GROUP = 256
TOK_DEV = 1024
SEQ_LEN = 32768
INNER_WIDTH = 3072
CAPACITY = 16
N_EXP = 8


def draw_head_decay_rate(key, part):
    lowest = math.log(5000.0 / SEQ_LEN ** 2)
    highest = math.log(8.0)
    spread = jax.random.uniform(key, (H,), jnp.float32)
    return jnp.exp(lowest + (highest - lowest) * spread)


def block_scale(rng, shape, split, smallest, top_value):
    factor_of = 1.0
    for position, parts in split:
        heights = jax.random.uniform(jax.random.fold_in(jax.random.fold_in(rng, 6), position), (parts,), jnp.float32, smallest / len(split), top_value / len(split))
        factor_of = factor_of * jnp.repeat(jnp.exp(heights), shape[position] // parts).reshape((-1,) + (1,) * (len(shape) - 1 - position))
    return factor_of


def shared_out(key, own, number, rows, number_of, top, reach, skew):
    ranking = jax.random.permutation(key, number_of)
    crowded, ordinary = load_shares(number_of, rows * top, reach, skew, True), load_shares(number_of, rows * top, reach, skew, False)
    places = jnp.arange(number_of)

    def named(sizes, turn):
        used = int((sizes > 0).sum())
        fixed = max(1, used // 4)
        moved = fixed + (places - fixed + turn * (used - fixed)) % max(1, number_of - fixed)
        return jnp.zeros((number_of,), jnp.int32).at[ranking[jnp.where(places < fixed, places, moved)]].set(jnp.asarray(sizes, jnp.int32))

    sizes = jnp.where(number % 4 == 0, named(crowded, number // 4), named(ordinary, number - number // 4 - 1))
    mixed = jax.random.permutation(jax.random.fold_in(own, 3), number_of)
    donor, receiver = mixed[0:number_of // 2 * 2:2], mixed[1:number_of // 2 * 2:2]
    slack = jnp.minimum(sizes[donor] - 1, reach - sizes[receiver]) // 2
    slack = jnp.where((donor == ranking[0]) | (receiver == ranking[0]) | (sizes[receiver] == 0), 0, jnp.maximum(slack, 0))
    moved = jax.random.randint(jax.random.fold_in(own, 4), (number_of // 2,), 0, 1 << 20) % (slack + 1)
    sizes = sizes.at[donor].add(-moved).at[receiver].add(moved)
    items = jnp.searchsorted(jnp.cumsum(sizes), jnp.arange(rows * top), side="right").astype(jnp.int32)
    listing = items.reshape(top, rows).T
    listing = listing[jax.random.permutation(jax.random.fold_in(own, 1), rows)]
    turn = jax.random.randint(jax.random.fold_in(own, 2), (rows, 1), 0, top)
    return jnp.take_along_axis(listing, (jnp.arange(top)[None, :] + turn) % top, axis=1)


def load_shares(number_of, total, reach, lean, full):
    weights = [(1 << 20) // math.isqrt(rank ** lean) + 1 for rank in range(1, number_of + 1)]
    largest = reach if full else min(reach, max(-(-total // number_of), total * weights[0] // sum(weights)))
    least = 1 if total - largest >= number_of - 1 else 0
    holding, surplus = [largest] + [least] * (number_of - 1), total - largest - least * (number_of - 1)
    while surplus > 0:
        movable = [i for i in range(1, number_of) if holding[i] < largest] or [i for i in range(1, number_of) if holding[i] < reach]
        whole, left = sum([weights[i] for i in movable]), surplus
        for i in movable:
            more = min(reach - holding[i], max(1, left * weights[i] // whole), surplus)
            holding[i] = holding[i] + more
            surplus = surplus - more
    return np.array(holding)


def noise(rng, extent, scale, most, cuts=(), held_as=jnp.bfloat16):
    gain = block_scale(rng, extent, cuts, -0.22, 0.18) if cuts else 1.0
    array = jax.random.normal(rng, extent, jnp.float32) * scale * gain
    return jnp.minimum(jnp.maximum(array, -most), most).astype(held_as)


def setup_inputs(seed: int = 0) -> dict:
    keys = jax.random.split(jax.random.key(seed), 16)
    tokens = noise(keys[0], (SEQ_LEN, MODEL_WIDTH), 1.0, 6.0, ((0, 256),))
    routes_keys = jax.random.split(jax.random.fold_in(keys[1], 1), SEQ_LEN // (TOK_DEV // N_EXP))
    routes_turns = jax.random.permutation(jax.random.fold_in(keys[1], 3), SEQ_LEN // (TOK_DEV // N_EXP))
    routes = jax.vmap(lambda own, number: shared_out(jax.random.fold_in(keys[1], 2), own, number, TOK_DEV // N_EXP, ADAPTER_EXPERTS, 1, CAPACITY, 2))(routes_keys, routes_turns).reshape((SEQ_LEN, 1))
    gate_inner_weight = noise(keys[2], (MODEL_WIDTH, 2, INNER_WIDTH), MODEL_WIDTH ** -0.5, 0.125, ((2, 8),))
    state_map_weight = noise(keys[3], (MODEL_WIDTH, 2 * STATE), MODEL_WIDTH ** -0.5, 0.125)
    step_size_weight = noise(keys[4], (MODEL_WIDTH, H), MODEL_WIDTH ** -0.5, 0.125, ((1, 8),))
    adapter_down_weight = noise(keys[5], (MODEL_WIDTH, ADAPTER_EXPERTS * EXPERT_RANK), MODEL_WIDTH ** -0.5, 0.125, ((1, 8),))
    adapter_up_weight = noise(keys[6], (ADAPTER_EXPERTS * EXPERT_RANK, 2, INNER_WIDTH), (2 * EXPERT_RANK) ** -0.5, 1.5, ((2, 8),))
    inner_conv_taps = noise(keys[7], (KERNEL, INNER_WIDTH), KERNEL ** -0.5, 3.0, ((1, 8),), jnp.float32)
    state_map_taps = noise(keys[8], (KERNEL, 2 * STATE), KERNEL ** -0.5, 3.0, (), jnp.float32)
    inner_conv_bias = noise(keys[9], (INNER_WIDTH,), 0.5, 3.0, ((0, 8),), jnp.float32)
    state_map_conv_bias = noise(keys[10], (2 * STATE,), 0.5, 3.0, (), jnp.float32)
    step_size_bias = jnp.clip(-6.0 + 3.0 * jax.random.uniform(keys[11], (H,), jnp.float32) ** block_scale(keys[11], (H,), ((0, 8),), -0.2, 0.2), -6.0, -3.0)
    head_decay_rate = draw_head_decay_rate(jax.random.fold_in(keys[15], 71), 0)
    direct_head_scale = jnp.clip(0.5 + 1.5 * jax.random.uniform(keys[13], (H,), jnp.float32) ** block_scale(keys[13], (H,), ((0, 8),), -0.2, 0.2), 0.5, 2.0)
    gated_norm_scale = jnp.clip(1.0 + 0.1 * jax.random.normal(keys[14], (INNER_WIDTH,), jnp.float32), 0.5, 1.5)
    return dict(tokens=tokens, routes=routes, gate_inner_weight=gate_inner_weight, state_map_weight=state_map_weight, step_size_weight=step_size_weight, adapter_down_weight=adapter_down_weight, adapter_up_weight=adapter_up_weight, inner_conv_taps=inner_conv_taps, state_map_taps=state_map_taps, inner_conv_bias=inner_conv_bias, state_map_conv_bias=state_map_conv_bias, step_size_bias=step_size_bias, head_decay_rate=head_decay_rate, direct_head_scale=direct_head_scale, gated_norm_scale=gated_norm_scale)


HIGH = lax.Precision.HIGHEST

def block_step(state, items):
    inner, bmap, cmap, step, decay = items
    cumul = jnp.cumsum(decay, axis=0)
    length = decay.shape[0]
    rows = lax.broadcasted_iota(jnp.int32, (length, length), 0)
    cols = lax.broadcasted_iota(jnp.int32, (length, length), 1)
    causal = (rows >= cols)[:, :, None]
    differ = jnp.where(causal, cumul[:, None, :] - cumul[None, :, :], 0.0)
    segment = jnp.where(causal, jnp.exp(differ), 0.0)
    gram = jnp.dot(cmap, bmap.T, precision=HIGH)
    weights = gram[:, :, None] * segment * step[None, :, :]
    output = jnp.einsum('ijh,jhp->ihp', weights, inner, precision=HIGH)
    output = output + jnp.exp(cumul)[:, :, None] * jnp.einsum('in,hnp->ihp', cmap, state, precision=HIGH)
    final = cumul[-1]
    carried = jnp.exp(final[None, :] - cumul) * step
    update = jnp.einsum('jn,jhp->hnp', bmap, carried[:, :, None] * inner, precision=HIGH)
    return (jnp.exp(final)[:, None, None] * state + update, output)

def run_blocks(inner, bmap, cmap, step, decay, state, block):
    total = inner.shape[0]
    count_blocks = total // block
    items = (inner.reshape(count_blocks, block, inner.shape[1], inner.shape[2]), bmap.reshape(count_blocks, block, bmap.shape[1]), cmap.reshape(count_blocks, block, cmap.shape[1]), step.reshape(count_blocks, block, step.shape[1]), decay.reshape(count_blocks, block, decay.shape[1]))
    final, output = lax.scan(block_step, state, items)
    return (final, output.reshape(total, inner.shape[1], inner.shape[2]))

def causal_conv(extended, weights, bias):
    length = extended.shape[0] - weights.shape[0] + 1
    output = bias[None, :] + jnp.zeros((length, weights.shape[1]), jnp.float32)
    for shift_idx in range(weights.shape[0]):
        output = output + weights[shift_idx][None, :] * extended[shift_idx:shift_idx + length]
    return jax.nn.silu(output)

def pick_ranks(partial_columns, route, first, experts, width):
    column_expert = first + lax.broadcasted_iota(jnp.int32, (experts * width,), 0) // width
    masked = jnp.where(route[:, None] == column_expert[None, :], partial_columns, 0.0)
    return lax.optimization_barrier(jnp.sum(masked.reshape(partial_columns.shape[0], experts, width), axis=1))

def lift_ranks(ranks, route, experts):
    width = ranks.shape[1]
    column_expert = lax.broadcasted_iota(jnp.int32, (experts * width,), 0) // width
    repeated_tiles = jnp.tile(ranks, (1, experts))
    return jnp.where(route[:, None] == column_expert[None, :], repeated_tiles, jnp.zeros_like(repeated_tiles))

def reference(tokens, routes, gate_inner_weight, state_map_weight, step_size_weight, adapter_down_weight, adapter_up_weight, inner_conv_taps, state_map_taps, inner_conv_bias, state_map_conv_bias, step_size_bias, head_decay_rate, direct_head_scale, gated_norm_scale):
    route = routes[:, 0]
    length = tokens.shape[0]
    partial_columns = jnp.dot(tokens, adapter_down_weight, preferred_element_type=jnp.float32)
    ranks = pick_ranks(partial_columns, route, 0, ADAPTER_EXPERTS, EXPERT_RANK).astype(jnp.bfloat16)
    raised_values = lift_ranks(ranks, route, ADAPTER_EXPERTS)
    gate_inner_values = jnp.dot(tokens, gate_inner_weight.reshape(MODEL_WIDTH, 2 * INNER_WIDTH), preferred_element_type=jnp.float32)
    gate_inner_values = gate_inner_values + jnp.dot(raised_values, adapter_up_weight.reshape(ADAPTER_EXPERTS * EXPERT_RANK, 2 * INNER_WIDTH), preferred_element_type=jnp.float32)
    gate = gate_inner_values[:, :INNER_WIDTH]
    inner = gate_inner_values[:, INNER_WIDTH:]
    bc_raw = jnp.dot(tokens, state_map_weight, preferred_element_type=jnp.float32)
    dt_raw = jnp.dot(tokens, step_size_weight, preferred_element_type=jnp.float32)
    margin = KERNEL - 1
    xconv = causal_conv(jnp.pad(inner, ((margin, 0), (0, 0))), inner_conv_taps, inner_conv_bias)
    bconv = causal_conv(jnp.pad(bc_raw, ((margin, 0), (0, 0))), state_map_taps, state_map_conv_bias)
    bmap = bconv[:, :STATE]
    cmap = bconv[:, STATE:]
    step = jax.nn.softplus(dt_raw + step_size_bias[None, :])
    decay = -head_decay_rate[None, :] * step
    heads_in = xconv.reshape(length, H, HEADDIM)
    start = jnp.zeros((H, STATE, HEADDIM), jnp.float32)
    final, output = run_blocks(heads_in, bmap, cmap, step, decay, start, GROUP)
    output = output + direct_head_scale[None, :, None] * heads_in
    gated = output.reshape(length, INNER_WIDTH) * jax.nn.silu(gate)
    meansq = lax.optimization_barrier(jnp.mean(gated * gated, axis=1, keepdims=True))
    return (gated * lax.rsqrt(meansq + 1e-05) * gated_norm_scale[None, :]).astype(jnp.bfloat16)
```

```python
import functools

import jax
import jax.numpy as jnp
from jax import lax
from jax.experimental import pallas as pl
from jax.experimental.pallas import tpu as pltpu
from jax.sharding import PartitionSpec as P

MODEL = 2560
STATE = 128
HEADS = 6
COLS = 384
RANK = 8
BLOCK = 128
N_EXP = 8
N_SEQ = 32
ROWS = 1024
INNER_WIDTH = 3072
SEG = 144
PIECES = ((128, 16), (0, 32), (32, 32), (64, 32), (96, 32))
F32, BF16 = jnp.float32, jnp.bfloat16
NT = (((1,), (1,)), ((), ()))
NN = (((1,), (0,)), ((), ()))


def dot(a, b, dims=NN):
    return lax.dot_general(a, b, dims, preferred_element_type=F32)


def split(a):
    hi = a.astype(BF16)
    return hi, (a - hi.astype(F32)).astype(BF16)


def dot3(a, b, dims=NN):
    (ah, al), (bh, bl) = a, b
    return dot(ah, bh, dims) + (dot(ah, bl, dims) + dot(al, bh, dims))


def silu(v):
    return v / (1.0 + jnp.exp(-v))


def lane_row(ref, width):
    lane = lax.broadcasted_iota(jnp.int32, (1, 128 if width == 1 else HEADS * width), 1) // width
    row = jnp.zeros(lane.shape, F32)
    for h in range(HEADS):
        row = jnp.where(lane == h, ref[h], row)
    return row


def kernel(
    tok_hbm, routes_ref, wgi_hbm, wbc_hbm, dt_ref, down_hbm, up_ref,
    taps_ref, btaps_ref, bias_ref, bbias_ref, sbias_ref, rate_ref, direct_ref, norm_ref,
    out_ref,
    tall, routes, wgi, wbc, ddt, zg, zi, zb, sd, rimx, rimb,
    cc, ybuf, ec, f1, r1, o2, r2, ebuf, sq, r3, scl,
    lsem, rsem, ssem, fsem, csem, rtr, rts, rimr, rims, s1, v1, s2, v2, s3, v3,
):
    e, s = lax.axis_index("exp"), lax.axis_index("seq")
    y, c = e // 2, e % 2
    yp, ym, yo = (y + 1) % 4, (y + 3) % 4, (y + 2) % 4
    plus, minus, mate = yp * 2 + c, ym * 2 + c, y * 2 + 1 - c

    loads = [
        pltpu.make_async_copy(tok_hbm, tall.at[e, pl.ds(0, 128)], lsem.at[0]),
        pltpu.make_async_copy(down_hbm, tall.at[e, pl.ds(128, 16)], lsem.at[1]),
        pltpu.make_async_copy(wgi_hbm, wgi, lsem.at[2]),
        pltpu.make_async_copy(wbc_hbm, wbc, lsem.at[3]),
    ]
    for load in loads:
        load.start()

    barrier = pltpu.get_barrier_semaphore()
    for d in range(1, N_EXP):
        pl.semaphore_signal(barrier, inc=1, device_id={"exp": (e + d) % N_EXP})

    @pl.loop(1, N_SEQ)
    def _(d):
        pl.semaphore_signal(barrier, inc=1, device_id={"seq": (s + d) % N_SEQ})

    routes[e] = routes_ref[...]
    ddt[...] = jnp.zeros_like(ddt)
    ddt[pl.ds(128, HEADS), :] = dt_ref[...]
    loads[0].wait()
    loads[1].wait()
    pl.semaphore_wait(barrier, N_EXP - 1 + N_SEQ - 1)

    def piece(b, k):
        first, size = PIECES[k]
        return tall.at[b, pl.ds(first, size)]

    def push(b, k, to, sem):
        copy = pltpu.make_async_remote_copy(
            src_ref=piece(b, k), dst_ref=piece(b, k), send_sem=sem, recv_sem=rsem.at[b, k],
            device_id={"exp": to},
        )
        copy.start()
        sent.append(copy)

    def landed(b, k):
        pltpu.make_async_remote_copy(
            src_ref=piece(b, k), dst_ref=piece(b, k), send_sem=lsem.at[0], recv_sem=rsem.at[b, k],
            device_id={"exp": mate},
        ).wait_recv()

    sent = []
    for d in range(1, N_EXP):
        copy = pltpu.make_async_remote_copy(
            src_ref=routes_ref, dst_ref=routes.at[e], send_sem=rts.at[d], recv_sem=rtr.at[e],
            device_id={"exp": (e + d) % N_EXP},
        )
        copy.start()
        sent.append(copy)
    for k, j in zip((0, 1, 2, 3, 4), (0, 3, 4, 1, 2)):
        push(e, k, plus, ssem.at[0, k])
        push(e, j, minus, ssem.at[1, j])
        push(e, k, mate, ssem.at[2, k])

    def take(b, k, slot, forward=None):
        landed(b, k)
        if forward is not None:
            push(b, k, forward, fsem.at[k])
        push(b, k, mate, csem.at[slot, k])

    bm, bp, bo = ym * 2 + c, yp * 2 + c, yo * 2 + c
    take(bm, 0, 0, plus)
    take(bp, 0, 1)
    take(bo, 0, 2)
    others = [y * 2 + 1 - c, ym * 2 + 1 - c, yp * 2 + 1 - c, yo * 2 + 1 - c]
    for b in others:
        landed(b, 0)
    for d in range(1, N_EXP):
        b = (e + d) % N_EXP
        pltpu.make_async_remote_copy(
            src_ref=routes_ref, dst_ref=routes.at[b], send_sem=lsem.at[0], recv_sem=rtr.at[b],
            device_id={"exp": mate},
        ).wait_recv()
    for b in range(N_EXP):
        ddt[pl.ds(16 * b, 16), :] = tall[b, pl.ds(128, 16), :]
    loads[2].wait()
    loads[3].wait()

    expert_of_lane = lax.broadcasted_iota(jnp.int32, (BLOCK, 128), 1) // RANK

    def project(b):
        t = tall[b, pl.ds(0, BLOCK), :]
        row = pl.multiple_of(b * BLOCK, BLOCK)
        aux = dot(t, ddt[...], NT)
        sd[pl.ds(row, BLOCK), :] = aux[:, 128:]
        route = jnp.broadcast_to(routes[b].astype(F32), (BLOCK, 128)).T.astype(jnp.int32)
        lifted = jnp.where(route == expert_of_lane, aux[:, :128], 0.0).astype(BF16)
        zg[pl.ds(row, BLOCK), :] = dot(t, wgi[:, :COLS]) + dot(lifted, up_ref[:, :COLS])
        zi[pl.ds(row + 8, BLOCK), :] = dot(t, wgi[:, COLS:]) + dot(lifted, up_ref[:, COLS:])
        zb[pl.ds(row + 8, BLOCK), :] = dot(t, wbc[...])

    def project_all(blocks):
        for b in blocks:
            project(b)

    project_all([e])
    for k in (1, 2, 3, 4):
        landed(others[0], k)
    project_all([others[0]])
    take(bm, 1, 0, plus)
    take(bp, 3, 1, minus)
    take(bm, 2, 0, plus)
    take(bp, 4, 1, minus)
    for k, j in ((3, 1), (4, 2)):
        take(bm, k, 0)
        take(bp, j, 1)
    project_all([bm, bp])
    for b in others[1:3]:
        for k in (1, 2, 3, 4):
            landed(b, k)
    project_all(others[1:3])
    for k in (1, 3, 2, 4):
        take(bo, k, 2)
    project_all([bo])
    for k in (1, 2, 3, 4):
        landed(others[3], k)
    project_all([others[3]])

    def rim_copies():
        return [
            pltpu.make_async_remote_copy(
                src_ref=zi.at[pl.ds(ROWS, 8)], dst_ref=rimx, send_sem=rims.at[0], recv_sem=rimr.at[0],
                device_id={"seq": (s + 1) % N_SEQ},
            ),
            pltpu.make_async_remote_copy(
                src_ref=zb.at[pl.ds(ROWS, 8)], dst_ref=rimb, send_sem=rims.at[1], recv_sem=rimr.at[1],
                device_id={"seq": (s + 1) % N_SEQ},
            ),
        ]

    for copy in rim_copies():
        copy.start()

    sbias, rate = lane_row(sbias_ref, 1), lane_row(rate_ref, 1)
    direct = lane_row(direct_ref, 64)
    ri = lax.broadcasted_iota(jnp.int32, (BLOCK, BLOCK), 0)
    ci = lax.broadcasted_iota(jnp.int32, (BLOCK, BLOCK), 1)
    causal = ri >= ci
    left = ci < 64

    def conv(window, taps, bias):
        acc = bias
        for j in range(4):
            acc = acc + taps[j : j + 1, :] * window[5 + j : 5 + j + BLOCK, :]
        return silu(acc)

    def local(k, carry):
        state, offset = carry
        row = pl.multiple_of(k * BLOCK, BLOCK)
        xc = conv(zi[pl.ds(row, BLOCK + 8), :], taps_ref, bias_ref[...][None, :])
        bc = conv(zb[pl.ds(row, BLOCK + 8), :], btaps_ref, bbias_ref[...][None, :])
        raw = sd[pl.ds(row, BLOCK), :]
        raw = jnp.concatenate([raw, jnp.zeros((BLOCK, 128 - raw.shape[1]), F32)], 1) + sbias
        step = jnp.maximum(raw, 0.0) + jnp.log1p(jnp.exp(-jnp.abs(raw)))
        decay = -rate * step
        cum = lax.dot_general(
            causal.astype(F32), decay, NN, precision=lax.Precision.HIGHEST, preferred_element_type=F32
        )
        cum_t, step_t = cum.T, step.T
        bmap, cmap = bc[:, :STATE], bc[:, STATE:]
        b2, c2 = split(bmap), split(cmap)
        gram = dot3(c2, b2, NT)
        b_t = bmap.T
        inter = dot3(c2, split(state))
        cc[0, pl.ds(row, BLOCK), :] = c2[0]
        cc[1, pl.ds(row, BLOCK), :] = c2[1]
        ys, us, ecs, tots = [], [], [], []
        for p in range(3):
            ws, bs, cols, tot = [], [], [], []
            for h in (2 * p, 2 * p + 1):
                ch = jnp.broadcast_to(cum[:, h : h + 1], (BLOCK, BLOCK))
                rh = cum_t[h : h + 1, :]
                th = cum[BLOCK - 1 : BLOCK, h : h + 1]
                seg = jnp.exp(jnp.where(causal, ch - rh, -1e30))
                sh = step_t[h : h + 1, :]
                ws.append(gram * seg * sh)
                bs.append(b_t * (jnp.exp(th - rh) * sh))
                cols.append(ch)
                tot.append(jnp.broadcast_to(th, (1, 128)))
            lhs = jnp.concatenate([jnp.concatenate(ws, 1), jnp.concatenate(bs, 1)], 0)
            xp = xc[:, 128 * p : 128 * p + 128]
            rhs = jnp.concatenate([jnp.where(left, xp, 0.0), jnp.where(left, 0.0, xp)], 0)
            both = dot3(split(lhs), split(rhs))
            ecp = jnp.exp(jnp.where(left, cols[0], cols[1]))
            ys.append(both[:BLOCK] + ecp * inter[:, 128 * p : 128 * p + 128])
            us.append(both[BLOCK:])
            ecs.append(ecp)
            tots.append(jnp.exp(jnp.where(left[:1], tot[0], tot[1])))
        tot = jnp.concatenate(tots, 1)
        ybuf[pl.ds(row, BLOCK), :] = jnp.concatenate(ys, 1) + direct * xc
        ec[pl.ds(row, BLOCK), :] = jnp.concatenate(ecs, 1) * offset
        return tot * state + jnp.concatenate(us, 1), offset * tot

    for copy in rim_copies():
        copy.wait()
    started = s > 0
    zi[pl.ds(0, 8), :] = jnp.where(started, rimx[...], 0.0)
    zb[pl.ds(0, 8), :] = jnp.where(started, rimb[...], 0.0)

    state, total = lax.fori_loop(
        0, ROWS // BLOCK, local, (jnp.zeros((STATE, COLS), F32), jnp.ones((1, COLS), F32))
    )

    for j in range(N_SEQ):
        f1[j, pl.ds(0, 4), :] = state[4 * j : 4 * j + 4, :]
        f1[j, pl.ds(4, 1), :] = total

    def first(d):
        to = (s + d) % N_SEQ
        return pltpu.make_async_remote_copy(
            src_ref=f1.at[to], dst_ref=r1.at[s], send_sem=s1.at[d], recv_sem=v1.at[s], device_id={"seq": to}
        )

    def first_in(d):
        at = (s + d) % N_SEQ
        return pltpu.make_async_remote_copy(
            src_ref=f1.at[at], dst_ref=r1.at[at], send_sem=s1.at[d], recv_sem=v1.at[at], device_id={"seq": at}
        )

    @pl.loop(1, N_SEQ)
    def _(d):
        first(d).start()

    r1[s] = f1[s]

    @pl.loop(1, N_SEQ)
    def _(d):
        first_in(d).wait_recv()

    run = jnp.zeros((4, COLS), F32)
    for r in range(N_SEQ):
        o2[r] = run
        run = run * r1[r, pl.ds(4, 1), :] + r1[r, pl.ds(0, 4), :]

    def second(d):
        to = (s + d) % N_SEQ
        return pltpu.make_async_remote_copy(
            src_ref=o2.at[to], dst_ref=r2.at[s], send_sem=s2.at[d], recv_sem=v2.at[s], device_id={"seq": to}
        )

    def second_in(d):
        at = (s + d) % N_SEQ
        return pltpu.make_async_remote_copy(
            src_ref=o2.at[at], dst_ref=r2.at[at], send_sem=s2.at[d], recv_sem=v2.at[at], device_id={"seq": at}
        )

    @pl.loop(1, N_SEQ)
    def _(d):
        second(d).start()

    r2[s] = o2[s]

    @pl.loop(0, ROWS // BLOCK)
    def _(k):
        row = pl.multiple_of(k * BLOCK, BLOCK)
        zg[pl.ds(row, BLOCK), :] = silu(zg[pl.ds(row, BLOCK), :])

    @pl.loop(1, N_SEQ)
    def _(d):
        second_in(d).wait_recv()

    for j in range(N_SEQ):
        ebuf[pl.ds(4 * j, 4), :] = r2[j]
    entering = split(ebuf[...])
    ones = jnp.ones((8, COLS), BF16)

    @pl.loop(0, ROWS // BLOCK)
    def _(k):
        row = pl.multiple_of(k * BLOCK, BLOCK)
        at = pl.ds(row, BLOCK)
        far = dot3((cc[0, at, :], cc[1, at, :]), entering)
        gated = (ybuf[at, :] + ec[at, :] * far) * zg[at, :]
        ybuf[at, :] = gated
        qh, ql = split(gated * gated)
        sq[k] = (dot(ones, qh, NT) + dot(ones, ql, NT))[:1, :]

    def third(d):
        to = (e + d) % N_EXP
        return pltpu.make_async_remote_copy(
            src_ref=sq, dst_ref=r3.at[e], send_sem=s3.at[d], recv_sem=v3.at[e], device_id={"exp": to}
        )

    def third_in(d):
        at = (e + d) % N_EXP
        return pltpu.make_async_remote_copy(
            src_ref=sq, dst_ref=r3.at[at], send_sem=s3.at[d], recv_sem=v3.at[at], device_id={"exp": at}
        )

    for d in range(1, N_EXP):
        third(d).start()
    r3[e] = sq[...]
    for d in range(1, N_EXP):
        third_in(d).wait_recv()
    scl[...] = lax.rsqrt(jnp.sum(r3[...], axis=0) / INNER_WIDTH + 1e-05)
    gain = norm_ref[...][None, :]

    @pl.loop(0, ROWS // BLOCK)
    def _(k):
        at = pl.ds(pl.multiple_of(k * BLOCK, BLOCK), BLOCK)
        scale = jnp.broadcast_to(scl[k], (BLOCK, 128)).T
        scale = jnp.concatenate([scale] * 3, 1)
        out_ref[at, :] = (ybuf[at, :] * scale * gain).astype(BF16)

    for copy in sent:
        copy.wait_send()

    @pl.loop(1, N_SEQ)
    def _(d):
        first(d).wait_send()
        second(d).wait_send()

    for d in range(1, N_EXP):
        third(d).wait_send()


def body(
    tokens, routes, gate_inner_weight, state_map_weight, step_size_weight, adapter_down_weight,
    adapter_up_weight, inner_conv_taps, state_map_taps, inner_conv_bias, state_map_conv_bias,
    step_size_bias, head_decay_rate, direct_head_scale, gated_norm_scale,
):
    vmem, smem, anyw = (
        pl.BlockSpec(memory_space=pltpu.VMEM),
        pl.BlockSpec(memory_space=pltpu.SMEM),
        pl.BlockSpec(memory_space=pl.ANY),
    )
    dma = pltpu.SemaphoreType.DMA
    return pl.pallas_call(
        kernel,
        out_shape=jax.ShapeDtypeStruct((ROWS, COLS), BF16),
        in_specs=[anyw, vmem, anyw, anyw, vmem, anyw, vmem] + [vmem] * 4 + [smem] * 3 + [vmem],
        out_specs=vmem,
        scratch_shapes=[
            pltpu.VMEM((N_EXP, SEG, MODEL), BF16),
            pltpu.VMEM((N_EXP, 1, 128), jnp.int32),
            pltpu.VMEM((MODEL, 2 * COLS), BF16),
            pltpu.VMEM((MODEL, 2 * STATE), BF16),
            pltpu.VMEM((SEG, MODEL), BF16),
            pltpu.VMEM((ROWS, COLS), F32),
            pltpu.VMEM((ROWS + 8, COLS), F32),
            pltpu.VMEM((ROWS + 8, 2 * STATE), F32),
            pltpu.VMEM((ROWS, 16), F32),
            pltpu.VMEM((8, COLS), F32),
            pltpu.VMEM((8, 2 * STATE), F32),
            pltpu.VMEM((2, ROWS, STATE), BF16),
            pltpu.VMEM((ROWS, COLS), F32),
            pltpu.VMEM((ROWS, COLS), F32),
            pltpu.VMEM((N_SEQ, 5, COLS), F32),
            pltpu.VMEM((N_SEQ, 5, COLS), F32),
            pltpu.VMEM((N_SEQ, 4, COLS), F32),
            pltpu.VMEM((N_SEQ, 4, COLS), F32),
            pltpu.VMEM((STATE, COLS), F32),
            pltpu.VMEM((8, 1, 128), F32),
            pltpu.VMEM((N_EXP, 8, 1, 128), F32),
            pltpu.VMEM((8, 1, 128), F32),
            dma((4,)),
            dma((N_EXP, 5)),
            dma((3, 5)),
            dma((5,)),
            dma((3, 5)),
            dma((N_EXP,)),
            dma((N_EXP,)),
            dma((2,)),
            dma((2,)),
            dma((N_SEQ,)),
            dma((N_SEQ,)),
            dma((N_SEQ,)),
            dma((N_SEQ,)),
            dma((N_EXP,)),
            dma((N_EXP,)),
        ],
        compiler_params=pltpu.CompilerParams(
            collective_id=0, has_side_effects=True, vmem_limit_bytes=62 * 1024 * 1024
        ),
    )(
        tokens, routes.T, gate_inner_weight.reshape(MODEL, 2 * COLS), state_map_weight,
        step_size_weight.T, adapter_down_weight.T, adapter_up_weight.reshape(128, 2 * COLS),
        inner_conv_taps, state_map_taps, inner_conv_bias, state_map_conv_bias,
        step_size_bias, head_decay_rate, direct_head_scale, gated_norm_scale,
    )


def solution(mesh):
    both = ("seq", "exp")
    in_specs = (
        P(both, None),
        P(both, None),
        P(None, None, "exp"),
        P(),
        P(None, "exp"),
        P(None, "exp"),
        P(None, None, "exp"),
        P(None, "exp"),
        P(),
        P("exp"),
        P(),
        P("exp"),
        P("exp"),
        P("exp"),
        P("exp"),
    )
    return jax.shard_map(
        body, mesh=mesh, in_specs=in_specs, out_specs=P("seq", "exp"), check_vma=False
    )
```

```python
import functools

import jax
import jax.numpy as jnp
from jax import lax
from jax.experimental import pallas as pl
from jax.experimental.pallas import tpu as pltpu
from jax.sharding import PartitionSpec as P

MODEL = 2560
STATE = 128
HEADS = 6
COLS = 384
RANK = 8
BLOCK = 128
N_EXP = 8
N_SEQ = 32
ROWS = 1024
INNER_WIDTH = 3072
SEG = 144
PIECES = ((128, 16), (0, 32), (32, 32), (64, 32), (96, 32))
F32, BF16 = jnp.float32, jnp.bfloat16
NT = (((1,), (1,)), ((), ()))
NN = (((1,), (0,)), ((), ()))


def dot(a, b, dims=NN):
    return lax.dot_general(a, b, dims, preferred_element_type=F32)


def split(a):
    hi = a.astype(BF16)
    return hi, (a - hi.astype(F32)).astype(BF16)


def dot3(a, b, dims=NN):
    (ah, al), (bh, bl) = a, b
    return dot(ah, bh, dims) + (dot(ah, bl, dims) + dot(al, bh, dims))


def silu(v):
    return v / (1.0 + jnp.exp(-v))


def lane_row(ref, width):
    lane = lax.broadcasted_iota(jnp.int32, (1, 128 if width == 1 else HEADS * width), 1) // width
    row = jnp.zeros(lane.shape, F32)
    for h in range(HEADS):
        row = jnp.where(lane == h, ref[h], row)
    return row


def kernel(
    tok_hbm, routes_hbm, wgi_hbm, wbc_hbm, dt_hbm, down_hbm, up3_hbm,
    taps_hbm, btaps_hbm, bias_hbm, bbias_hbm, sbias_ref, rate_ref, direct_ref, norm_hbm,
    out_ref,
    routes_ref, dt_ref, up3_ref, taps_ref, btaps_ref, bias_ref, bbias_ref, norm_ref, tall, routes, wraw, wgi, wbc, ddt, up, zg, zi, zb, sd, rimx, rimb,
    cc, ybuf, ec, xcb, bsp, cumb, cumt, stept, uu, tots, f1, r1, o2, r2, ebuf, sq, r3,
    lsem, rsem, ssem, fsem, csem, rtr, rts, rimr, rims, s1, v1, s2, v2, s3, v3,
):
    e, s = lax.axis_index("exp"), lax.axis_index("seq")
    y, c = e // 2, e % 2
    yp, ym, yo = (y + 1) % 4, (y + 3) % 4, (y + 2) % 4
    plus, minus, mate = yp * 2 + c, ym * 2 + c, y * 2 + 1 - c

    loads = [
        pltpu.make_async_copy(tok_hbm, tall.at[e, pl.ds(0, 128)], lsem.at[0]),
        pltpu.make_async_copy(down_hbm, tall.at[e, pl.ds(128, 16)], lsem.at[1]),
        pltpu.make_async_copy(wgi_hbm, wraw, lsem.at[2]),
        pltpu.make_async_copy(wbc_hbm, wbc, lsem.at[3]),
        pltpu.make_async_copy(routes_hbm, routes_ref, lsem.at[4]),
        pltpu.make_async_copy(dt_hbm, dt_ref, lsem.at[5]),
        pltpu.make_async_copy(up3_hbm, up3_ref, lsem.at[6]),
        pltpu.make_async_copy(taps_hbm, taps_ref, lsem.at[7]),
        pltpu.make_async_copy(btaps_hbm, btaps_ref, lsem.at[8]),
        pltpu.make_async_copy(bias_hbm, bias_ref, lsem.at[9]),
        pltpu.make_async_copy(bbias_hbm, bbias_ref, lsem.at[10]),
        pltpu.make_async_copy(norm_hbm, norm_ref, lsem.at[11]),
    ]
    for load in loads:
        load.start()

    barrier = pltpu.get_barrier_semaphore()
    for d in range(1, N_EXP):
        pl.semaphore_signal(barrier, inc=1, device_id={"exp": (e + d) % N_EXP})

    @pl.loop(1, N_SEQ)
    def _(d):
        pl.semaphore_signal(barrier, inc=1, device_id={"seq": (s + d) % N_SEQ})

    ddt[...] = jnp.zeros_like(ddt)
    for i in (0, 1, 4, 5, 6, 7, 8, 9, 10, 11):
        loads[i].wait()
    routes[e] = routes_ref[...]
    ddt[pl.ds(128, HEADS), :] = dt_ref[...]
    pl.semaphore_wait(barrier, N_EXP - 1 + N_SEQ - 1)

    def piece(b, k):
        first, size = PIECES[k]
        return tall.at[b, pl.ds(first, size)]

    def push(b, k, to, sem):
        copy = pltpu.make_async_remote_copy(
            src_ref=piece(b, k), dst_ref=piece(b, k), send_sem=sem, recv_sem=rsem.at[b, k],
            device_id={"exp": to},
        )
        copy.start()
        sent.append(copy)

    def landed(b, k):
        pltpu.make_async_remote_copy(
            src_ref=piece(b, k), dst_ref=piece(b, k), send_sem=lsem.at[0], recv_sem=rsem.at[b, k],
            device_id={"exp": mate},
        ).wait_recv()

    sent = []
    for d in range(1, N_EXP):
        copy = pltpu.make_async_remote_copy(
            src_ref=routes_ref, dst_ref=routes.at[e], send_sem=rts.at[d], recv_sem=rtr.at[e],
            device_id={"exp": (e + d) % N_EXP},
        )
        copy.start()
        sent.append(copy)
    for k in range(5):
        push(e, k, mate, ssem.at[2, k])
    push(e, 0, plus, ssem.at[0, 0])
    push(e, 0, minus, ssem.at[1, 0])
    push(e, 1, plus, ssem.at[0, 1])
    push(e, 3, minus, ssem.at[1, 3])

    def take(b, k, slot, forward=None):
        landed(b, k)
        if forward is not None:
            push(b, k, forward, fsem.at[k])
        push(b, k, mate, csem.at[slot, k])

    bm, bp, bo = ym * 2 + c, yp * 2 + c, yo * 2 + c
    others = [y * 2 + 1 - c, ym * 2 + 1 - c, yp * 2 + 1 - c, yo * 2 + 1 - c]

    loads[2].wait()
    loads[3].wait()

    @pl.loop(0, MODEL // 32)
    def _(i):
        at = pl.ds(pl.multiple_of(i * 32, 32), 32)
        wgi[at, :] = wraw[at, :, :].reshape(32, 2 * COLS)

    up[...] = up3_ref[...].reshape(128, 2 * COLS)

    expert_of_lane = lax.broadcasted_iota(jnp.int32, (BLOCK, 128), 1) // RANK

    def main(b):
        t = tall[b, pl.ds(0, BLOCK), :]
        row = pl.multiple_of(b * BLOCK, BLOCK)
        zg[pl.ds(row, BLOCK), :] = dot(t, wgi[:, :COLS])
        zi[pl.ds(row + 8, BLOCK), :] = dot(t, wgi[:, COLS:])
        zb[pl.ds(row + 8, BLOCK), :] = dot(t, wbc[...])

    def routed(b):
        t = tall[b, pl.ds(0, BLOCK), :]
        row = pl.multiple_of(b * BLOCK, BLOCK)
        aux = dot(t, ddt[...], NT)
        sd[pl.ds(row, BLOCK), :] = aux[:, 128:]
        route = jnp.broadcast_to(routes[b].astype(F32), (BLOCK, 128)).T.astype(jnp.int32)
        lifted = jnp.where(route == expert_of_lane, aux[:, :128], 0.0).astype(BF16)
        zg[pl.ds(row, BLOCK), :] += dot(lifted, up[:, :COLS])
        zi[pl.ds(row + 8, BLOCK), :] += dot(lifted, up[:, COLS:])

    take(bm, 0, 0, plus)
    for k in (2, 3, 4):
        push(e, k, plus, ssem.at[0, k])
    for k in (4, 1, 2):
        push(e, k, minus, ssem.at[1, k])
    take(bp, 0, 1)
    main(e)
    for k in (1, 2, 3, 4):
        landed(others[0], k)
    main(others[0])
    take(bm, 1, 0, plus)
    take(bp, 3, 1, minus)
    take(bo, 0, 2)
    for b in others:
        landed(b, 0)
    for d in range(1, N_EXP):
        b = (e + d) % N_EXP
        pltpu.make_async_remote_copy(
            src_ref=routes_ref, dst_ref=routes.at[b], send_sem=lsem.at[0], recv_sem=rtr.at[b],
            device_id={"exp": mate},
        ).wait_recv()
    for b in range(N_EXP):
        ddt[pl.ds(16 * b, 16), :] = tall[b, pl.ds(128, 16), :]
    routed(e)
    routed(others[0])
    take(bp, 4, 1, minus)
    take(bm, 2, 0, plus)

    sbias, rate = lane_row(sbias_ref, 1), lane_row(rate_ref, 1)
    direct = lane_row(direct_ref, 64)
    ri = lax.broadcasted_iota(jnp.int32, (BLOCK, BLOCK), 0)
    ci = lax.broadcasted_iota(jnp.int32, (BLOCK, BLOCK), 1)
    causal = ri >= ci
    lower = causal.astype(F32)
    left = ci < 64

    def conv(window, taps, bias):
        acc = bias
        for j in range(4):
            acc = acc + taps[j : j + 1, :] * window[5 + j : 5 + j + BLOCK, :]
        return silu(acc)

    def side_by_side(xp):
        return split(jnp.concatenate([jnp.where(left, xp, 0.0), jnp.where(left, 0.0, xp)], 0))

    def states(k):
        row = pl.multiple_of(k * BLOCK, BLOCK)
        at = pl.ds(row, BLOCK)
        xc = conv(zi[pl.ds(row, BLOCK + 8), :], taps_ref, bias_ref[...][None, :])
        bmap = conv(zb[pl.ds(row, BLOCK + 8), :STATE], btaps_ref[:, :STATE], bbias_ref[...][None, :STATE])
        raw = sd[at, :]
        raw = jnp.concatenate([raw, jnp.zeros((BLOCK, 128 - raw.shape[1]), F32)], 1) + sbias
        step = jnp.maximum(raw, 0.0) + jnp.log1p(jnp.exp(-jnp.abs(raw)))
        decay = -rate * step
        cum = lax.dot_general(
            lower, decay, NN, precision=lax.Precision.HIGHEST, preferred_element_type=F32
        )
        cum_t, step_t = cum.T[:8], step.T[:8]
        xcb[at, :] = xc
        bh, bl = split(bmap)
        bsp[0, at, :] = bh
        bsp[1, at, :] = bl
        cumb[at, :] = cum
        cumt[k] = cum_t
        stept[k] = step_t
        b_t = bmap.T
        us, ts = [], []
        for p in range(3):
            bs, tot = [], []
            for h in (2 * p, 2 * p + 1):
                th = cum[BLOCK - 1 : BLOCK, h : h + 1]
                bs.append(b_t * (jnp.exp(th - cum_t[h : h + 1, :]) * step_t[h : h + 1, :]))
                tot.append(jnp.broadcast_to(th, (1, 128)))
            us.append(dot3(split(jnp.concatenate(bs, 1)), side_by_side(xc[:, 128 * p : 128 * p + 128])))
            ts.append(jnp.exp(jnp.where(left[:1], tot[0], tot[1])))
        uu[k] = jnp.concatenate(us, 1)
        tots[k] = jnp.concatenate(ts, 1)

    def states_but_first(k):
        @pl.when(k != 0)
        def _():
            states(k)

    states_but_first(2 * y + 1)
    for k in (1, 2):
        take(bp, k, 1)
    main(bp)
    routed(bp)
    for k in (1, 2, 3, 4):
        landed(others[2], k)
    main(others[2])
    routed(others[2])
    for k in (3, 4):
        take(bm, k, 0)
    main(bm)
    routed(bm)
    for k in (1, 2, 3, 4):
        landed(others[1], k)
    main(others[1])
    routed(others[1])
    states_but_first(2 * yp)
    take(bo, 3, 2)
    states_but_first(2 * yp + 1)
    take(bo, 1, 2)
    states_but_first(2 * y)
    states_but_first(2 * ym + 1)
    for k in (4, 2):
        take(bo, k, 2)
    main(bo)
    routed(bo)
    for k in (1, 2, 3, 4):
        landed(others[3], k)
    main(others[3])
    routed(others[3])

    def rim_copies():
        return [
            pltpu.make_async_remote_copy(
                src_ref=zi.at[pl.ds(ROWS, 8)], dst_ref=rimx, send_sem=rims.at[0], recv_sem=rimr.at[0],
                device_id={"seq": (s + 1) % N_SEQ},
            ),
            pltpu.make_async_remote_copy(
                src_ref=zb.at[pl.ds(ROWS, 8)], dst_ref=rimb, send_sem=rims.at[1], recv_sem=rimr.at[1],
                device_id={"seq": (s + 1) % N_SEQ},
            ),
        ]

    for copy in rim_copies():
        copy.start()

    states_but_first(2 * yo)
    states_but_first(2 * yo + 1)
    states_but_first(2 * ym)
    for copy in rim_copies():
        copy.wait()
    started = s > 0
    zi[pl.ds(0, 8), :] = jnp.where(started, rimx[...], 0.0)
    zb[pl.ds(0, 8), :] = jnp.where(started, rimb[...], 0.0)
    states(0)

    state, total = jnp.zeros((STATE, COLS), F32), jnp.ones((1, COLS), F32)
    for k in range(ROWS // BLOCK):
        update, tot = uu[k], tots[k]
        uu[k] = state
        tots[k] = total
        state, total = tot * state + update, total * tot

    spare = jnp.concatenate([total[:, 128 * p : 128 * p + 128] for p in (0, 1, 2, 2)], 0)
    for j in range(N_SEQ):
        f1[j] = jnp.concatenate([state[4 * j : 4 * j + 4, :], spare], 1)

    x, z = s % 4, s // 4
    offsets = sorted(
        ((i, j) for i in range(8) for j in range(4) if i or j),
        key=lambda o: -min(o[0], 8 - o[0]) - min(o[1], 4 - o[1]),
    )

    def away(d):
        i, j = offsets[d - 1]
        return (z + i) % 8 * 4 + (x + j) % 4

    def first(d):
        to = away(d)
        return pltpu.make_async_remote_copy(
            src_ref=f1.at[to], dst_ref=r1.at[s], send_sem=s1.at[d], recv_sem=v1.at[s], device_id={"seq": to}
        )

    def first_in(d):
        at = (s + d) % N_SEQ
        return pltpu.make_async_remote_copy(
            src_ref=f1.at[at], dst_ref=r1.at[at], send_sem=s1.at[d], recv_sem=v1.at[at], device_id={"seq": at}
        )

    for d in range(1, N_SEQ):
        first(d).start()

    r1[s] = f1[s]

    @pl.loop(0, ROWS // BLOCK)
    def _(k):
        row = pl.multiple_of(k * BLOCK, BLOCK)
        at = pl.ds(row, BLOCK)
        cmap = conv(zb[pl.ds(row, BLOCK + 8), STATE:], btaps_ref[:, STATE:], bbias_ref[...][None, STATE:])
        c2 = split(cmap)
        cc[0, at, :], cc[1, at, :] = c2
        gram = dot3(c2, (bsp[0, at, :], bsp[1, at, :]), NT)
        inter = dot3(c2, split(uu[k]))
        cum, cum_t, step_t, xc = cumb[at, :], cumt[k], stept[k], xcb[at, :]
        ys, ecs = [], []
        for p in range(3):
            ws, cols = [], []
            for h in (2 * p, 2 * p + 1):
                ch = jnp.broadcast_to(cum[:, h : h + 1], (BLOCK, BLOCK))
                seg = jnp.exp(jnp.where(causal, ch - cum_t[h : h + 1, :], -1e30))
                ws.append(gram * seg * step_t[h : h + 1, :])
                cols.append(ch)
            near = dot3(split(jnp.concatenate(ws, 1)), side_by_side(xc[:, 128 * p : 128 * p + 128]))
            ecp = jnp.exp(jnp.where(left, cols[0], cols[1]))
            ys.append(near + ecp * inter[:, 128 * p : 128 * p + 128])
            ecs.append(ecp)
        ybuf[at, :] = jnp.concatenate(ys, 1) + direct * xc
        ec[at, :] = jnp.concatenate(ecs, 1) * tots[k]

    @pl.loop(1, N_SEQ)
    def _(d):
        first_in(d).wait_recv()

    run = [jnp.zeros((4, 128), F32)] * 3
    for r in range(N_SEQ):
        o2[r] = jnp.concatenate(run, 1)
        come = r1[r]
        run = [
            run[p] * come[p : p + 1, COLS:] + come[:, 128 * p : 128 * p + 128] for p in range(3)
        ]

    def second(d):
        to = away(d)
        return pltpu.make_async_remote_copy(
            src_ref=o2.at[to], dst_ref=r2.at[s], send_sem=s2.at[d], recv_sem=v2.at[s], device_id={"seq": to}
        )

    def second_in(d):
        at = (s + d) % N_SEQ
        return pltpu.make_async_remote_copy(
            src_ref=o2.at[at], dst_ref=r2.at[at], send_sem=s2.at[d], recv_sem=v2.at[at], device_id={"seq": at}
        )

    for d in range(1, N_SEQ):
        second(d).start()

    r2[s] = o2[s]

    @pl.loop(0, ROWS // BLOCK)
    def _(k):
        row = pl.multiple_of(k * BLOCK, BLOCK)
        zg[pl.ds(row, BLOCK), :] = silu(zg[pl.ds(row, BLOCK), :])

    @pl.loop(1, N_SEQ)
    def _(d):
        second_in(d).wait_recv()

    for j in range(N_SEQ):
        ebuf[pl.ds(4 * j, 4), :] = r2[j]
    entering = split(ebuf[...])

    def third(half, d):
        to = (e + d) % N_EXP
        return pltpu.make_async_remote_copy(
            src_ref=sq.at[half], dst_ref=r3.at[half, e], send_sem=s3.at[half, d],
            recv_sem=v3.at[half, e], device_id={"exp": to},
        )

    def third_in(half, d):
        at = (e + d) % N_EXP
        return pltpu.make_async_remote_copy(
            src_ref=sq.at[half], dst_ref=r3.at[half, at], send_sem=s3.at[half, d],
            recv_sem=v3.at[half, at], device_id={"exp": at},
        )

    for half in (0, 1):
        for k in (0, 2):
            at = pl.ds(512 * half + 128 * k, 2 * BLOCK)
            far = dot3((cc[0, at, :], cc[1, at, :]), entering)
            gated = (ybuf[at, :] + ec[at, :] * far) * zg[at, :]
            ybuf[at, :] = gated
            gated = gated * gated
            gated = gated[:, :128] + gated[:, 128:256] + gated[:, 256:]
            for i in (0, 1):
                sq[half, k + i] = jnp.sum(gated[128 * i : 128 * i + 128].T, axis=0, keepdims=True)
        for d in range(1, N_EXP):
            third(half, d).start()
    gain = norm_ref[...][None, :]
    for half in (0, 1):
        r3[half, e] = sq[half]
        for d in range(1, N_EXP):
            third_in(half, d).wait_recv()
        scale = lax.rsqrt(jnp.sum(r3[half], axis=0) / INNER_WIDTH + 1e-05)
        for k in range(4):
            at = pl.ds(512 * half + 128 * k, BLOCK)
            wide = jnp.broadcast_to(scale[k], (BLOCK, 128)).T
            wide = jnp.concatenate([wide] * 3, 1)
            out_ref[at, :] = (ybuf[at, :] * wide * gain).astype(BF16)

    for copy in sent:
        copy.wait_send()

    for d in range(1, N_SEQ):
        first(d).wait_send()
        second(d).wait_send()

    for half in (0, 1):
        for d in range(1, N_EXP):
            third(half, d).wait_send()


def body(
    tokens, routes, gate_inner_weight, state_map_weight, step_size_weight, adapter_down_weight,
    adapter_up_weight, inner_conv_taps, state_map_taps, inner_conv_bias, state_map_conv_bias,
    step_size_bias, head_decay_rate, direct_head_scale, gated_norm_scale,
):
    vmem, smem, hbm = (
        pl.BlockSpec(memory_space=pltpu.VMEM),
        pl.BlockSpec(memory_space=pltpu.SMEM),
        pl.BlockSpec(memory_space=pltpu.HBM),
    )
    dma = pltpu.SemaphoreType.DMA
    return pl.pallas_call(
        kernel,
        out_shape=jax.ShapeDtypeStruct((ROWS, COLS), BF16),
        in_specs=[hbm] * 11 + [smem] * 3 + [hbm],
        out_specs=vmem,
        scratch_shapes=[
            pltpu.VMEM((1, 128), jnp.int32),
            pltpu.VMEM((HEADS, MODEL), BF16),
            pltpu.VMEM((128, 2, COLS), BF16),
            pltpu.VMEM((4, COLS), F32),
            pltpu.VMEM((4, 2 * STATE), F32),
            pltpu.VMEM((COLS,), F32),
            pltpu.VMEM((2 * STATE,), F32),
            pltpu.VMEM((COLS,), F32),
            pltpu.VMEM((N_EXP, SEG, MODEL), BF16),
            pltpu.VMEM((N_EXP, 1, 128), jnp.int32),
            pltpu.VMEM((MODEL, 2, COLS), BF16),
            pltpu.VMEM((MODEL, 2 * COLS), BF16),
            pltpu.VMEM((MODEL, 2 * STATE), BF16),
            pltpu.VMEM((SEG, MODEL), BF16),
            pltpu.VMEM((128, 2 * COLS), BF16),
            pltpu.VMEM((ROWS, COLS), F32),
            pltpu.VMEM((ROWS + 8, COLS), F32),
            pltpu.VMEM((ROWS + 8, 2 * STATE), F32),
            pltpu.VMEM((ROWS, 16), F32),
            pltpu.VMEM((8, COLS), F32),
            pltpu.VMEM((8, 2 * STATE), F32),
            pltpu.VMEM((2, ROWS, STATE), BF16),
            pltpu.VMEM((ROWS, COLS), F32),
            pltpu.VMEM((ROWS, COLS), F32),
            pltpu.VMEM((ROWS, COLS), F32),
            pltpu.VMEM((2, ROWS, STATE), BF16),
            pltpu.VMEM((ROWS, 128), F32),
            pltpu.VMEM((8, 8, 128), F32),
            pltpu.VMEM((8, 8, 128), F32),
            pltpu.VMEM((8, STATE, COLS), F32),
            pltpu.VMEM((8, 1, COLS), F32),
            pltpu.VMEM((N_SEQ, 4, COLS + 128), F32),
            pltpu.VMEM((N_SEQ, 4, COLS + 128), F32),
            pltpu.VMEM((N_SEQ, 4, COLS), F32),
            pltpu.VMEM((N_SEQ, 4, COLS), F32),
            pltpu.VMEM((STATE, COLS), F32),
            pltpu.VMEM((2, 4, 1, 128), F32),
            pltpu.VMEM((2, N_EXP, 4, 1, 128), F32),
            dma((12,)),
            dma((N_EXP, 5)),
            dma((3, 5)),
            dma((5,)),
            dma((3, 5)),
            dma((N_EXP,)),
            dma((N_EXP,)),
            dma((2,)),
            dma((2,)),
            dma((N_SEQ,)),
            dma((N_SEQ,)),
            dma((N_SEQ,)),
            dma((N_SEQ,)),
            dma((2, N_EXP)),
            dma((2, N_EXP)),
        ],
        compiler_params=pltpu.CompilerParams(
            collective_id=0, has_side_effects=True, vmem_limit_bytes=62 * 1024 * 1024
        ),
    )(
        tokens, routes.T, gate_inner_weight, state_map_weight,
        step_size_weight.T, adapter_down_weight.T, adapter_up_weight,
        inner_conv_taps, state_map_taps, inner_conv_bias, state_map_conv_bias,
        step_size_bias, head_decay_rate, direct_head_scale, gated_norm_scale,
    )


def solution(mesh):
    both = ("seq", "exp")
    in_specs = (
        P(both, None),
        P(both, None),
        P(None, None, "exp"),
        P(),
        P(None, "exp"),
        P(None, "exp"),
        P(None, None, "exp"),
        P(None, "exp"),
        P(),
        P("exp"),
        P(),
        P("exp"),
        P("exp"),
        P("exp"),
        P("exp"),
    )
    return jax.shard_map(
        body, mesh=mesh, in_specs=in_specs, out_specs=P("seq", "exp"), check_vma=False
    )
```

```python
import functools

import jax
import jax.numpy as jnp
from jax import lax
from jax.experimental import pallas as pl
from jax.experimental.pallas import tpu as pltpu
from jax.sharding import PartitionSpec as P

MODEL = 2560
STATE = 128
HEADS = 6
COLS = 384
RANK = 8
BLOCK = 128
N_EXP = 8
N_SEQ = 32
ROWS = 1024
INNER_WIDTH = 3072
SEG = 144
PIECES = ((128, 16), (0, 32), (32, 32), (64, 32), (96, 32))
F32, BF16 = jnp.float32, jnp.bfloat16
NT = (((1,), (1,)), ((), ()))
NN = (((1,), (0,)), ((), ()))


def dot(a, b, dims=NN):
    return lax.dot_general(a, b, dims, preferred_element_type=F32)


def split(a):
    hi = a.astype(BF16)
    return hi, (a - hi.astype(F32)).astype(BF16)


def dot3(a, b, dims=NN):
    (ah, al), (bh, bl) = a, b
    return dot(ah, bh, dims) + (dot(ah, bl, dims) + dot(al, bh, dims))


def silu(v):
    return v / (1.0 + jnp.exp(-v))


def lane_row(ref, width):
    lane = lax.broadcasted_iota(jnp.int32, (1, 128 if width == 1 else HEADS * width), 1) // width
    row = jnp.zeros(lane.shape, F32)
    for h in range(HEADS):
        row = jnp.where(lane == h, ref[h], row)
    return row


def kernel(
    tok_hbm, routes_hbm, wgi_hbm, wbc_hbm, dt_hbm, down_hbm, up3_hbm,
    taps_hbm, btaps_hbm, bias_hbm, bbias_hbm, sbias_ref, rate_ref, direct_ref, norm_hbm,
    out_ref,
    routes_ref, dt_ref, up3_ref, taps_ref, btaps_ref, bias_ref, bbias_ref, norm_ref, tall, routes, wraw, wgi, wbc, ddt, up, zg, zi, zb, sd, rimx, rimb,
    cc, ybuf, ec, xcb, bsp, cumb, cumt, stept, uu, tots, f1, r1, o2, r2, ebuf, sq, r3,
    lsem, rsem, ssem, fsem, csem, rtr, rts, rimr, rims, s1, v1, s2, v2, s3, v3,
):
    e, s = lax.axis_index("exp"), lax.axis_index("seq")
    y, c = e // 2, e % 2
    yp, ym, yo = (y + 1) % 4, (y + 3) % 4, (y + 2) % 4
    plus, minus, mate = yp * 2 + c, ym * 2 + c, y * 2 + 1 - c

    loads = [
        pltpu.make_async_copy(tok_hbm, tall.at[e, pl.ds(0, 128)], lsem.at[0]),
        pltpu.make_async_copy(down_hbm, tall.at[e, pl.ds(128, 16)], lsem.at[1]),
        pltpu.make_async_copy(wgi_hbm, wraw, lsem.at[2]),
        pltpu.make_async_copy(wbc_hbm, wbc, lsem.at[3]),
        pltpu.make_async_copy(routes_hbm, routes_ref, lsem.at[4]),
        pltpu.make_async_copy(dt_hbm, dt_ref, lsem.at[5]),
        pltpu.make_async_copy(up3_hbm, up3_ref, lsem.at[6]),
        pltpu.make_async_copy(taps_hbm, taps_ref, lsem.at[7]),
        pltpu.make_async_copy(btaps_hbm, btaps_ref, lsem.at[8]),
        pltpu.make_async_copy(bias_hbm, bias_ref, lsem.at[9]),
        pltpu.make_async_copy(bbias_hbm, bbias_ref, lsem.at[10]),
        pltpu.make_async_copy(norm_hbm, norm_ref, lsem.at[11]),
    ]
    for load in loads:
        load.start()

    barrier = pltpu.get_barrier_semaphore()
    for d in range(1, N_EXP):
        pl.semaphore_signal(barrier, inc=1, device_id={"exp": (e + d) % N_EXP})

    @pl.loop(1, N_SEQ)
    def _(d):
        pl.semaphore_signal(barrier, inc=1, device_id={"seq": (s + d) % N_SEQ})

    ddt[...] = jnp.zeros_like(ddt)
    for i in (0, 1, 4, 5, 6, 7, 8, 9, 10, 11):
        loads[i].wait()
    routes[e] = routes_ref[...]
    ddt[pl.ds(128, HEADS), :] = dt_ref[...]
    pl.semaphore_wait(barrier, N_EXP - 1 + N_SEQ - 1)

    def piece(b, k):
        first, size = PIECES[k]
        return tall.at[b, pl.ds(first, size)]

    def push(b, k, to, sem):
        copy = pltpu.make_async_remote_copy(
            src_ref=piece(b, k), dst_ref=piece(b, k), send_sem=sem, recv_sem=rsem.at[b, k],
            device_id={"exp": to},
        )
        copy.start()
        sent.append(copy)

    def landed(b, k):
        pltpu.make_async_remote_copy(
            src_ref=piece(b, k), dst_ref=piece(b, k), send_sem=lsem.at[0], recv_sem=rsem.at[b, k],
            device_id={"exp": mate},
        ).wait_recv()

    sent = []
    for d in range(1, N_EXP):
        copy = pltpu.make_async_remote_copy(
            src_ref=routes_ref, dst_ref=routes.at[e], send_sem=rts.at[d], recv_sem=rtr.at[e],
            device_id={"exp": (e + d) % N_EXP},
        )
        copy.start()
        sent.append(copy)
    for k in range(5):
        push(e, k, mate, ssem.at[2, k])
    push(e, 0, plus, ssem.at[0, 0])
    push(e, 0, minus, ssem.at[1, 0])
    push(e, 1, plus, ssem.at[0, 1])
    push(e, 3, minus, ssem.at[1, 3])

    def take(b, k, slot, forward=None):
        landed(b, k)
        if forward is not None:
            push(b, k, forward, fsem.at[k])
        push(b, k, mate, csem.at[slot, k])

    bm, bp, bo = ym * 2 + c, yp * 2 + c, yo * 2 + c
    others = [y * 2 + 1 - c, ym * 2 + 1 - c, yp * 2 + 1 - c, yo * 2 + 1 - c]

    loads[2].wait()
    loads[3].wait()

    @pl.loop(0, MODEL // 32)
    def _(i):
        at = pl.ds(pl.multiple_of(i * 32, 32), 32)
        wgi[at, :] = wraw[at, :, :].reshape(32, 2 * COLS)

    up[...] = up3_ref[...].reshape(128, 2 * COLS)

    expert_of_lane = lax.broadcasted_iota(jnp.int32, (BLOCK, 128), 1) // RANK

    def main(b):
        t = tall[b, pl.ds(0, BLOCK), :]
        row = pl.multiple_of(b * BLOCK, BLOCK)
        zg[pl.ds(row, BLOCK), :] = dot(t, wgi[:, :COLS])
        zi[pl.ds(row + 8, BLOCK), :] = dot(t, wgi[:, COLS:])
        zb[pl.ds(row + 8, BLOCK), :] = dot(t, wbc[...])

    def routed(b):
        t = tall[b, pl.ds(0, BLOCK), :]
        row = pl.multiple_of(b * BLOCK, BLOCK)
        aux = dot(t, ddt[...], NT)
        sd[pl.ds(row, BLOCK), :] = aux[:, 128:]
        route = jnp.broadcast_to(routes[b].astype(F32), (BLOCK, 128)).T.astype(jnp.int32)
        lifted = jnp.where(route == expert_of_lane, aux[:, :128], 0.0).astype(BF16)
        zg[pl.ds(row, BLOCK), :] += dot(lifted, up[:, :COLS])
        zi[pl.ds(row + 8, BLOCK), :] += dot(lifted, up[:, COLS:])

    take(bm, 0, 0, plus)
    for k in (2, 3, 4):
        push(e, k, plus, ssem.at[0, k])
    for k in (4, 1, 2):
        push(e, k, minus, ssem.at[1, k])
    take(bp, 0, 1)
    main(e)
    for k in (1, 2, 3, 4):
        landed(others[0], k)
    main(others[0])
    take(bm, 1, 0, plus)
    take(bp, 3, 1, minus)
    take(bo, 0, 2)
    for b in others:
        landed(b, 0)
    for d in range(1, N_EXP):
        b = (e + d) % N_EXP
        pltpu.make_async_remote_copy(
            src_ref=routes_ref, dst_ref=routes.at[b], send_sem=lsem.at[0], recv_sem=rtr.at[b],
            device_id={"exp": mate},
        ).wait_recv()
    for b in range(N_EXP):
        ddt[pl.ds(16 * b, 16), :] = tall[b, pl.ds(128, 16), :]
    routed(e)
    routed(others[0])
    take(bp, 4, 1, minus)
    take(bm, 2, 0, plus)

    sbias, rate = lane_row(sbias_ref, 1), lane_row(rate_ref, 1)
    direct = lane_row(direct_ref, 64)
    ri = lax.broadcasted_iota(jnp.int32, (BLOCK, BLOCK), 0)
    ci = lax.broadcasted_iota(jnp.int32, (BLOCK, BLOCK), 1)
    causal = ri >= ci
    lower = causal.astype(F32).astype(BF16)
    left = ci < 64

    def conv(window, taps, bias):
        acc = bias
        for j in range(4):
            acc = acc + taps[j : j + 1, :] * window[5 + j : 5 + j + BLOCK, :]
        return silu(acc)

    def side_by_side(xp):
        return split(jnp.concatenate([jnp.where(left, xp, 0.0), jnp.where(left, 0.0, xp)], 0))

    def states(k):
        row = pl.multiple_of(k * BLOCK, BLOCK)
        at = pl.ds(row, BLOCK)
        xc = conv(zi[pl.ds(row, BLOCK + 8), :], taps_ref, bias_ref[...][None, :])
        bmap = conv(zb[pl.ds(row, BLOCK + 8), :STATE], btaps_ref[:, :STATE], bbias_ref[...][None, :STATE])
        raw = sd[at, :]
        raw = jnp.concatenate([raw, jnp.zeros((BLOCK, 128 - raw.shape[1]), F32)], 1) + sbias
        step = jnp.maximum(raw, 0.0) + jnp.log1p(jnp.exp(-jnp.abs(raw)))
        decay = -rate * step
        d1, rest = split(decay)[0], decay - split(decay)[0].astype(F32)
        d2, d3 = split(rest)
        cum = dot(lower, d1) + (dot(lower, d2) + dot(lower, d3))
        cum_t, step_t = cum.T[:8], step.T[:8]
        xcb[at, :] = xc
        bh, bl = split(bmap)
        bsp[0, at, :] = bh
        bsp[1, at, :] = bl
        cumb[at, :] = cum
        cumt[k] = cum_t
        stept[k] = step_t
        b_t = bmap.T
        us, ts = [], []
        for p in range(3):
            bs, tot = [], []
            for h in (2 * p, 2 * p + 1):
                th = cum[BLOCK - 1 : BLOCK, h : h + 1]
                bs.append(b_t * (jnp.exp(th - cum_t[h : h + 1, :]) * step_t[h : h + 1, :]))
                tot.append(jnp.broadcast_to(th, (1, 128)))
            us.append(dot3(split(jnp.concatenate(bs, 1)), side_by_side(xc[:, 128 * p : 128 * p + 128])))
            ts.append(jnp.exp(jnp.where(left[:1], tot[0], tot[1])))
        uu[k] = jnp.concatenate(us, 1)
        tots[k] = jnp.concatenate(ts, 1)

    def states_but_first(k):
        @pl.when(k != 0)
        def _():
            states(k)

    states_but_first(2 * y + 1)
    for k in (1, 2):
        take(bp, k, 1)
    main(bp)
    routed(bp)
    for k in (1, 2, 3, 4):
        landed(others[2], k)
    main(others[2])
    routed(others[2])
    for k in (3, 4):
        take(bm, k, 0)
    main(bm)
    routed(bm)
    for k in (1, 2, 3, 4):
        landed(others[1], k)
    main(others[1])
    routed(others[1])
    states_but_first(2 * yp)
    take(bo, 3, 2)
    states_but_first(2 * yp + 1)
    take(bo, 1, 2)
    states_but_first(2 * y)
    states_but_first(2 * ym + 1)
    for k in (4, 2):
        take(bo, k, 2)
    main(bo)
    routed(bo)
    for k in (1, 2, 3, 4):
        landed(others[3], k)
    main(others[3])
    routed(others[3])

    def rim_copies():
        return [
            pltpu.make_async_remote_copy(
                src_ref=zi.at[pl.ds(ROWS, 8)], dst_ref=rimx, send_sem=rims.at[0], recv_sem=rimr.at[0],
                device_id={"seq": (s + 1) % N_SEQ},
            ),
            pltpu.make_async_remote_copy(
                src_ref=zb.at[pl.ds(ROWS, 8)], dst_ref=rimb, send_sem=rims.at[1], recv_sem=rimr.at[1],
                device_id={"seq": (s + 1) % N_SEQ},
            ),
        ]

    for copy in rim_copies():
        copy.start()

    states_but_first(2 * yo)
    states_but_first(2 * yo + 1)
    states_but_first(2 * ym)
    for copy in rim_copies():
        copy.wait()
    started = s > 0
    zi[pl.ds(0, 8), :] = jnp.where(started, rimx[...], 0.0)
    zb[pl.ds(0, 8), :] = jnp.where(started, rimb[...], 0.0)
    states(0)

    state, total = jnp.zeros((STATE, COLS), F32), jnp.ones((1, COLS), F32)
    for k in range(ROWS // BLOCK):
        update, tot = uu[k], tots[k]
        uu[k] = state
        tots[k] = total
        state, total = tot * state + update, total * tot

    spare = jnp.concatenate([total[:, 128 * p : 128 * p + 128] for p in (0, 1, 2, 2)], 0)
    for j in range(N_SEQ):
        f1[j] = jnp.concatenate([state[4 * j : 4 * j + 4, :], spare], 1)

    x, z = s % 4, s // 4
    offsets = sorted(
        ((i, j) for i in range(8) for j in range(4) if i or j),
        key=lambda o: -min(o[0], 8 - o[0]) - min(o[1], 4 - o[1]),
    )

    def away(d):
        i, j = offsets[d - 1]
        return (z + i) % 8 * 4 + (x + j) % 4

    def first(d):
        to = away(d)
        return pltpu.make_async_remote_copy(
            src_ref=f1.at[to], dst_ref=r1.at[s], send_sem=s1.at[d], recv_sem=v1.at[s], device_id={"seq": to}
        )

    def first_in(d):
        at = (s + d) % N_SEQ
        return pltpu.make_async_remote_copy(
            src_ref=f1.at[at], dst_ref=r1.at[at], send_sem=s1.at[d], recv_sem=v1.at[at], device_id={"seq": at}
        )

    for d in range(1, N_SEQ):
        first(d).start()

    r1[s] = f1[s]

    def inside(k):
        row = pl.multiple_of(k * BLOCK, BLOCK)
        at = pl.ds(row, BLOCK)
        cmap = conv(zb[pl.ds(row, BLOCK + 8), STATE:], btaps_ref[:, STATE:], bbias_ref[...][None, STATE:])
        c2 = split(cmap)
        cc[0, at, :], cc[1, at, :] = c2
        gram = dot3(c2, (bsp[0, at, :], bsp[1, at, :]), NT)
        inter = dot3(c2, split(uu[k]))
        cum, cum_t, step_t, xc = cumb[at, :], cumt[k], stept[k], xcb[at, :]
        ys, ecs = [], []
        for p in range(3):
            ws, cols = [], []
            for h in (2 * p, 2 * p + 1):
                ch = jnp.broadcast_to(cum[:, h : h + 1], (BLOCK, BLOCK))
                seg = jnp.exp(jnp.where(causal, ch - cum_t[h : h + 1, :], -1e30))
                ws.append(gram * seg * step_t[h : h + 1, :])
                cols.append(ch)
            near = dot3(split(jnp.concatenate(ws, 1)), side_by_side(xc[:, 128 * p : 128 * p + 128]))
            ecp = jnp.exp(jnp.where(left, cols[0], cols[1]))
            ys.append(near + ecp * inter[:, 128 * p : 128 * p + 128])
            ecs.append(ecp)
        ybuf[at, :] = jnp.concatenate(ys, 1) + direct * xc
        ec[at, :] = jnp.concatenate(ecs, 1) * tots[k]

    @pl.loop(0, 6)
    def _(k):
        inside(k)

    @pl.loop(1, N_SEQ)
    def _(d):
        first_in(d).wait_recv()

    run = [jnp.zeros((4, 128), F32)] * 3
    for r in range(N_SEQ):
        o2[r] = jnp.concatenate(run, 1).astype(BF16)
        come = r1[r]
        run = [
            run[p] * come[p : p + 1, COLS:] + come[:, 128 * p : 128 * p + 128] for p in range(3)
        ]

    def second(d):
        to = away(d)
        return pltpu.make_async_remote_copy(
            src_ref=o2.at[to], dst_ref=r2.at[s], send_sem=s2.at[d], recv_sem=v2.at[s], device_id={"seq": to}
        )

    def second_in(d):
        at = (s + d) % N_SEQ
        return pltpu.make_async_remote_copy(
            src_ref=o2.at[at], dst_ref=r2.at[at], send_sem=s2.at[d], recv_sem=v2.at[at], device_id={"seq": at}
        )

    for d in range(1, N_SEQ):
        second(d).start()

    r2[s] = o2[s]

    @pl.loop(6, ROWS // BLOCK)
    def _(k):
        inside(k)

    @pl.loop(0, ROWS // BLOCK)
    def _(k):
        row = pl.multiple_of(k * BLOCK, BLOCK)
        zg[pl.ds(row, BLOCK), :] = silu(zg[pl.ds(row, BLOCK), :])

    @pl.loop(1, N_SEQ)
    def _(d):
        second_in(d).wait_recv()

    for j in range(N_SEQ):
        ebuf[pl.ds(4 * j, 4), :] = r2[j].astype(F32)
    entering = ebuf[...].astype(BF16)

    def third(half, d):
        to = (e + d) % N_EXP
        return pltpu.make_async_remote_copy(
            src_ref=sq.at[half], dst_ref=r3.at[half, e], send_sem=s3.at[half, d],
            recv_sem=v3.at[half, e], device_id={"exp": to},
        )

    def third_in(half, d):
        at = (e + d) % N_EXP
        return pltpu.make_async_remote_copy(
            src_ref=sq.at[half], dst_ref=r3.at[half, at], send_sem=s3.at[half, d],
            recv_sem=v3.at[half, at], device_id={"exp": at},
        )

    for half in (0, 1):
        for k in (0, 2):
            at = pl.ds(512 * half + 128 * k, 2 * BLOCK)
            far = dot(cc[0, at, :], entering) + dot(cc[1, at, :], entering)
            gated = (ybuf[at, :] + ec[at, :] * far) * zg[at, :]
            ybuf[at, :] = gated
            gated = gated * gated
            gated = gated[:, :128] + gated[:, 128:256] + gated[:, 256:]
            for i in (0, 1):
                sq[half, k + i] = jnp.sum(gated[128 * i : 128 * i + 128].T, axis=0, keepdims=True)
        for d in range(1, N_EXP):
            third(half, d).start()
    gain = norm_ref[...][None, :]
    for half in (0, 1):
        r3[half, e] = sq[half]
        for d in range(1, N_EXP):
            third_in(half, d).wait_recv()
        scale = lax.rsqrt(jnp.sum(r3[half], axis=0) / INNER_WIDTH + 1e-05)
        for k in range(4):
            at = pl.ds(512 * half + 128 * k, BLOCK)
            wide = jnp.broadcast_to(scale[k], (BLOCK, 128)).T
            wide = jnp.concatenate([wide] * 3, 1)
            out_ref[at, :] = (ybuf[at, :] * wide * gain).astype(BF16)

    for copy in sent:
        copy.wait_send()

    for d in range(1, N_SEQ):
        first(d).wait_send()
        second(d).wait_send()

    for half in (0, 1):
        for d in range(1, N_EXP):
            third(half, d).wait_send()


def body(
    tokens, routes, gate_inner_weight, state_map_weight, step_size_weight, adapter_down_weight,
    adapter_up_weight, inner_conv_taps, state_map_taps, inner_conv_bias, state_map_conv_bias,
    step_size_bias, head_decay_rate, direct_head_scale, gated_norm_scale,
):
    vmem, smem, hbm = (
        pl.BlockSpec(memory_space=pltpu.VMEM),
        pl.BlockSpec(memory_space=pltpu.SMEM),
        pl.BlockSpec(memory_space=pltpu.HBM),
    )
    dma = pltpu.SemaphoreType.DMA
    return pl.pallas_call(
        kernel,
        out_shape=jax.ShapeDtypeStruct((ROWS, COLS), BF16),
        in_specs=[hbm] * 11 + [smem] * 3 + [hbm],
        out_specs=vmem,
        scratch_shapes=[
            pltpu.VMEM((1, 128), jnp.int32),
            pltpu.VMEM((HEADS, MODEL), BF16),
            pltpu.VMEM((128, 2, COLS), BF16),
            pltpu.VMEM((4, COLS), F32),
            pltpu.VMEM((4, 2 * STATE), F32),
            pltpu.VMEM((COLS,), F32),
            pltpu.VMEM((2 * STATE,), F32),
            pltpu.VMEM((COLS,), F32),
            pltpu.VMEM((N_EXP, SEG, MODEL), BF16),
            pltpu.VMEM((N_EXP, 1, 128), jnp.int32),
            pltpu.VMEM((MODEL, 2, COLS), BF16),
            pltpu.VMEM((MODEL, 2 * COLS), BF16),
            pltpu.VMEM((MODEL, 2 * STATE), BF16),
            pltpu.VMEM((SEG, MODEL), BF16),
            pltpu.VMEM((128, 2 * COLS), BF16),
            pltpu.VMEM((ROWS, COLS), F32),
            pltpu.VMEM((ROWS + 8, COLS), F32),
            pltpu.VMEM((ROWS + 8, 2 * STATE), F32),
            pltpu.VMEM((ROWS, 16), F32),
            pltpu.VMEM((8, COLS), F32),
            pltpu.VMEM((8, 2 * STATE), F32),
            pltpu.VMEM((2, ROWS, STATE), BF16),
            pltpu.VMEM((ROWS, COLS), F32),
            pltpu.VMEM((ROWS, COLS), F32),
            pltpu.VMEM((ROWS, COLS), F32),
            pltpu.VMEM((2, ROWS, STATE), BF16),
            pltpu.VMEM((ROWS, 128), F32),
            pltpu.VMEM((8, 8, 128), F32),
            pltpu.VMEM((8, 8, 128), F32),
            pltpu.VMEM((8, STATE, COLS), F32),
            pltpu.VMEM((8, 1, COLS), F32),
            pltpu.VMEM((N_SEQ, 4, COLS + 128), F32),
            pltpu.VMEM((N_SEQ, 4, COLS + 128), F32),
            pltpu.VMEM((N_SEQ, 4, COLS), BF16),
            pltpu.VMEM((N_SEQ, 4, COLS), BF16),
            pltpu.VMEM((STATE, COLS), F32),
            pltpu.VMEM((2, 4, 1, 128), F32),
            pltpu.VMEM((2, N_EXP, 4, 1, 128), F32),
            dma((12,)),
            dma((N_EXP, 5)),
            dma((3, 5)),
            dma((5,)),
            dma((3, 5)),
            dma((N_EXP,)),
            dma((N_EXP,)),
            dma((2,)),
            dma((2,)),
            dma((N_SEQ,)),
            dma((N_SEQ,)),
            dma((N_SEQ,)),
            dma((N_SEQ,)),
            dma((2, N_EXP)),
            dma((2, N_EXP)),
        ],
        compiler_params=pltpu.CompilerParams(
            collective_id=0, has_side_effects=True, vmem_limit_bytes=62 * 1024 * 1024
        ),
    )(
        tokens, routes.T, gate_inner_weight, state_map_weight,
        step_size_weight.T, adapter_down_weight.T, adapter_up_weight,
        inner_conv_taps, state_map_taps, inner_conv_bias, state_map_conv_bias,
        step_size_bias, head_decay_rate, direct_head_scale, gated_norm_scale,
    )


def solution(mesh):
    both = ("seq", "exp")
    in_specs = (
        P(both, None),
        P(both, None),
        P(None, None, "exp"),
        P(),
        P(None, "exp"),
        P(None, "exp"),
        P(None, None, "exp"),
        P(None, "exp"),
        P(),
        P("exp"),
        P(),
        P("exp"),
        P("exp"),
        P("exp"),
        P("exp"),
    )
    return jax.shard_map(
        body, mesh=mesh, in_specs=in_specs, out_specs=P("seq", "exp"), check_vma=False
    )
```
